32 devices in a mesh: dp: 1 (over z), cp: 32 (over y, x, core).
Axes of the slice: x: 4, y: 4, z: 1, core: 2. Of those that a mesh axis runs over, the one named last changes fastest.
The devices are a block of a 4x4x8 slice.
Arguments:
- hidden: bfloat16 [6, 3072, 3584], P('dp', 'cp')
- positions: int32 [6, 3072], P('dp', 'cp')
- w_q: bfloat16 [3584, 16, 256], replicated
- w_k: bfloat16 [3584, 8, 256], replicated
- w_v: bfloat16 [3584, 8, 256], replicated
- w_o: bfloat16 [16, 256, 3584], replicated
Outputs:
- output: bfloat16 [6, 3072, 3584], P('dp', 'cp')
All inputs are finite; a program needn't handle non-finite values.
Results may differ from the reference program's by a relative error of at most 0.00861.
Values are sent between devices in bfloat16 or wider.
A program may use at most 768 MiB of HBM per device.

```python
import jax
import jax.numpy as jnp
from jax import lax

BATCH = 6
SEQ = 3072
D = 3584
HEADS = 16
KV_HEADS = 8
HEAD = 256

ROPE_BASE = 500000.0
Q_PER_KV = HEADS // KV_HEADS


def setup_inputs(seed: int = 0, part: int = 0) -> dict:
    part_key = jax.random.fold_in(jax.random.key(seed), part)
    k_noise, k_coef, k_phase, k_step, k_first = jax.random.split(part_key, 5)
    k_wq, k_wk, k_wv, k_wo = jax.random.split(jax.random.key(seed + 1), 4)
    time_grid = jnp.arange(SEQ, dtype=jnp.float32) / SEQ
    mode_ids = jnp.arange(1, 5, dtype=jnp.float32)
    phases = jax.random.uniform(k_phase, (BATCH, 4), jnp.float32, 0.0, 6.2831853)
    wave_vals = jnp.cos(6.2831853 * time_grid[None, :, None] * mode_ids[None, None, :] + phases[:, None, :])
    mode_coef = 0.6 * jax.random.normal(k_coef, (BATCH, 4, D), jnp.float32)
    slow_part = jnp.einsum('bsm,bmd->bsd', wave_vals, mode_coef)
    noise_part = 0.6 * jax.random.normal(k_noise, (BATCH, SEQ, D), jnp.float32)
    hidden = (slow_part + noise_part).astype(jnp.bfloat16)
    step_sizes = jax.random.randint(k_step, (BATCH, SEQ), 1, 5)
    first_pos = jax.random.randint(k_first, (BATCH, 1), 0, 4)
    positions = (first_pos + jnp.cumsum(step_sizes, axis=1) - step_sizes[:, :1]).astype(jnp.int32)
    w_q = (jax.random.normal(k_wq, (D, HEADS, HEAD), jnp.float32) * D ** -0.5).astype(jnp.bfloat16)
    w_k = (jax.random.normal(k_wk, (D, KV_HEADS, HEAD), jnp.float32) * D ** -0.5).astype(jnp.bfloat16)
    w_v = (jax.random.normal(k_wv, (D, KV_HEADS, HEAD), jnp.float32) * (2.0 * D ** -0.5)).astype(jnp.bfloat16)
    w_o = (jax.random.normal(k_wo, (HEADS, HEAD, D), jnp.float32) * (HEADS * HEAD) ** -0.5).astype(jnp.bfloat16)
    return {'hidden': hidden, 'positions': positions, 'w_q': w_q, 'w_k': w_k, 'w_v': w_v, 'w_o': w_o}


def rope_tables(positions):
    inv_freq = ROPE_BASE ** (-jnp.arange(0, HEAD, 2, dtype=jnp.float32) / HEAD)
    angles = positions.astype(jnp.float32)[..., None] * inv_freq
    angles = jnp.concatenate([angles, angles], axis=-1)
    return jnp.cos(angles)[:, :, None, :], jnp.sin(angles)[:, :, None, :]


def rope_apply(in_vals, cos_tab, sin_tab):
    half_dim = in_vals.shape[-1] // 2
    val_f32 = in_vals.astype(jnp.float32)
    rotated = jnp.concatenate([-val_f32[..., half_dim:], val_f32[..., :half_dim]], axis=-1)
    return (val_f32 * cos_tab + rotated * sin_tab).astype(jnp.bfloat16)


def reference(hidden, positions, w_q, w_k, w_v, w_o):
    x_float = hidden.astype(jnp.float32)
    queries = jnp.einsum('bsd,dhe->bshe', x_float, w_q.astype(jnp.float32)).astype(jnp.bfloat16)
    k_proj = jnp.einsum('bsd,dhe->bshe', x_float, w_k.astype(jnp.float32)).astype(jnp.bfloat16)
    values = jnp.einsum('bsd,dhe->bshe', x_float, w_v.astype(jnp.float32)).astype(jnp.bfloat16)
    cos_tab, sin_tab = rope_tables(positions)
    queries = rope_apply(queries, cos_tab, sin_tab)
    k_rot = rope_apply(k_proj, cos_tab, sin_tab)
    q_block = 16
    n_blocks = SEQ // q_block
    q_blocks = queries.reshape(BATCH, n_blocks, q_block, KV_HEADS, Q_PER_KV, HEAD).transpose(1, 0, 2, 3, 4, 5)
    pos_blocks = positions.reshape(BATCH, n_blocks, q_block).transpose(1, 0, 2)
    k_float = k_rot.astype(jnp.float32)
    v_float = values.astype(jnp.float32)
    sm_scale = HEAD ** -0.5

    def one_block(block_args):
        q_blk, pos_blk = block_args
        scores = jnp.einsum('bqkge,bske->bkgqs', q_blk.astype(jnp.float32), k_float) * sm_scale
        allowed = positions[:, None, None, None, :] <= pos_blk[:, None, None, :, None]
        scores = jnp.where(allowed, scores, -jnp.inf)
        row_max = jnp.max(scores, axis=-1, keepdims=True)
        p_weights = jnp.exp(scores - row_max)
        row_sum = jnp.sum(p_weights, axis=-1)
        out_acc = jnp.einsum('bkgqs,bske->bqkge', p_weights.astype(jnp.bfloat16).astype(jnp.float32), v_float)
        return (out_acc / row_sum.transpose(0, 3, 1, 2)[..., None]).astype(jnp.bfloat16)

    attn_blocks = lax.map(one_block, (q_blocks, pos_blocks))
    attn_out = attn_blocks.transpose(1, 0, 2, 3, 4, 5).reshape(BATCH, SEQ, HEADS, HEAD)
    proj_out = jnp.einsum('bshe,hed->bsd', attn_out.astype(jnp.float32), w_o.astype(jnp.float32))
    return (x_float + proj_out).astype(jnp.bfloat16)
```

```python
import functools

import jax
import jax.numpy as jnp
from jax import lax
from jax.experimental import pallas as pl
from jax.experimental.pallas import tpu as pltpu
from jax.sharding import PartitionSpec as P

ROPE_BASE = 500000.0
LOG2E = 1.4426950408889634


def rope_tables(positions, head_dim):
    inv_freq = ROPE_BASE ** (-jnp.arange(0, head_dim, 2, dtype=jnp.float32) / head_dim)
    angles = positions.astype(jnp.float32)[..., None] * inv_freq
    angles = jnp.concatenate([angles, angles], axis=-1)
    return jnp.cos(angles)[:, :, None, :], jnp.sin(angles)[:, :, None, :]


def rope_apply(in_vals, cos_tab, sin_tab):
    half_dim = in_vals.shape[-1] // 2
    val_f32 = in_vals.astype(jnp.float32)
    rotated = jnp.concatenate([-val_f32[..., half_dim:], val_f32[..., :half_dim]], axis=-1)
    return (val_f32 * cos_tab + rotated * sin_tab).astype(jnp.bfloat16)


def project(hidden, weights):
    return jnp.einsum('bsd,dhe->bshe', hidden, weights, preferred_element_type=jnp.float32).astype(jnp.bfloat16)


def flash_kernel(blk, q_ref, mine_ref, o_ref, kv_ref, copy_sem, send_sem, recv_sem):
    seq, head_dim = q_ref.shape
    me = lax.axis_index('cp')
    core = lax.rem(me, 2)
    partner = {'cp': me + 1 - 2 * core}
    barrier = pltpu.get_barrier_semaphore()
    pl.semaphore_signal(barrier, inc=1, device_id=partner, device_id_type=pl.DeviceIdType.MESH)
    keep = pltpu.make_async_copy(mine_ref, kv_ref.at[core], copy_sem)
    keep.start()
    pl.semaphore_wait(barrier, 1)
    share = pltpu.make_async_remote_copy(
        src_ref=mine_ref,
        dst_ref=kv_ref.at[core],
        send_sem=send_sem,
        recv_sem=recv_sem,
        device_id=partner,
        device_id_type=pl.DeviceIdType.MESH,
    )
    share.start()
    keep.wait()
    share.wait()
    scale = (head_dim ** -0.5) * LOG2E
    for c in range(seq // blk):
        rows, width = pl.ds(c * blk, blk), (c + 1) * blk
        scores = lax.dot_general(
            q_ref[rows, :], kv_ref[0, pl.ds(0, width), :], (((1,), (1,)), ((), ())), preferred_element_type=jnp.float32
        )
        row_ids = lax.broadcasted_iota(jnp.int32, (blk, width), 0) + c * blk
        col_ids = lax.broadcasted_iota(jnp.int32, (blk, width), 1)
        scores = jnp.where(col_ids <= row_ids, scores, -jnp.inf)
        row_max = jnp.max(scores, axis=1, keepdims=True)
        p_weights = jnp.exp2((scores - row_max) * scale)
        row_sum = jnp.sum(p_weights, axis=1, keepdims=True)
        out = jnp.dot(p_weights.astype(jnp.bfloat16), kv_ref[1, pl.ds(0, width), :], preferred_element_type=jnp.float32)
        o_ref[rows, :] = (out / row_sum).astype(o_ref.dtype)


def flash(queries, mine, collective_id):
    seq, head_dim = queries.shape
    blk = 256 if seq % 256 == 0 else 96
    return pl.pallas_call(
        functools.partial(flash_kernel, blk),
        out_shape=jax.ShapeDtypeStruct((seq, head_dim), jnp.bfloat16),
        in_specs=[pl.BlockSpec(memory_space=pltpu.VMEM), pl.BlockSpec(memory_space=pl.ANY)],
        out_specs=pl.BlockSpec(memory_space=pltpu.VMEM),
        scratch_shapes=[
            pltpu.VMEM((2, seq, head_dim), jnp.bfloat16),
            pltpu.SemaphoreType.DMA,
            pltpu.SemaphoreType.DMA,
            pltpu.SemaphoreType.DMA,
        ],
        compiler_params=pltpu.CompilerParams(collective_id=collective_id, has_side_effects=True),
        cost_estimate=pl.CostEstimate(flops=2 * seq * seq * head_dim, bytes_accessed=8 * seq * head_dim, transcendentals=seq * seq // 2),
        name='flash',
    )(queries, mine)


def solution(mesh):
    cp_size = mesh.shape['cp']

    def per_device(hidden, positions, w_q, w_k, w_v, w_o):
        n_seq, tok_dev, width = hidden.shape
        n_heads, head_dim = w_q.shape[1], w_q.shape[2]
        n_kv = w_k.shape[1]
        per_round = cp_size // n_heads
        n_rounds = n_seq // per_round
        seq_len = cp_size * tok_dev
        cos_tab, sin_tab = rope_tables(positions, head_dim)

        def exchange(blocks):
            return lax.all_to_all(blocks.reshape(cp_size, tok_dev, head_dim), 'cp', 0, 0)

        k_rot = rope_apply(project(hidden, w_k), cos_tab, sin_tab).transpose(0, 2, 1, 3)
        values = project(hidden, w_v).transpose(0, 2, 1, 3)
        kv_send = jnp.stack([k_rot, values], axis=2)
        queries = rope_apply(project(hidden, w_q), cos_tab, sin_tab).transpose(0, 2, 1, 3)
        outs = []
        for r in range(n_rounds):
            part = slice(r * per_round, (r + 1) * per_round)
            kv_mine = exchange(kv_send[part])
            q_mine = exchange(queries[part])
            o_mine = flash(q_mine.reshape(seq_len, head_dim), kv_mine.reshape(seq_len, head_dim), r + 1)
            outs.append(exchange(o_mine).reshape(per_round, n_heads, tok_dev, head_dim))
        o_back = jnp.concatenate(outs, axis=0)
        proj_out = jnp.einsum('bhse,hed->bsd', o_back, w_o, preferred_element_type=jnp.float32)
        return (hidden.astype(jnp.float32) + proj_out).astype(jnp.bfloat16)

    rep_spec = P(None, None, None)
    return jax.shard_map(per_device, mesh=mesh, in_specs=(P('dp', 'cp', None), P('dp', 'cp'), rep_spec, rep_spec, rep_spec, rep_spec), out_specs=P('dp', 'cp', None), check_vma=False)
```

```python
import functools
import math

import jax
import jax.numpy as jnp
from jax import lax
from jax.experimental import pallas as pl
from jax.experimental.pallas import tpu as pltpu
from jax.sharding import PartitionSpec as P

ROPE_BASE = 500000.0
LOG2E = 1.4426950408889634


def rope_tables(positions, head_dim):
    inv_freq = ROPE_BASE ** (-jnp.arange(0, head_dim, 2, dtype=jnp.float32) / head_dim)
    angles = positions.astype(jnp.float32)[..., None] * inv_freq
    angles = jnp.concatenate([angles, angles], axis=-1)
    return jnp.cos(angles)[:, :, None, :], jnp.sin(angles)[:, :, None, :]


def rope_apply(in_vals, cos_tab, sin_tab):
    half_dim = in_vals.shape[-1] // 2
    val_f32 = in_vals.astype(jnp.float32)
    rotated = jnp.concatenate([-val_f32[..., half_dim:], val_f32[..., :half_dim]], axis=-1)
    return (val_f32 * cos_tab + rotated * sin_tab).astype(jnp.bfloat16)


def project(hidden, weights):
    return jnp.einsum('bsd,dhe->bshe', hidden, weights, preferred_element_type=jnp.float32).astype(jnp.bfloat16)


def peer_offsets(side):
    order = []
    for dy in range(side):
        for dx in range(side):
            for dc in range(2):
                for a, b in ((dy, dx), (-dy % side, -dx % side), (dx, dy), (-dx % side, -dy % side)):
                    if (a, b, dc) != (0, 0, 0) and (a, b, dc) not in order:
                        order.append((a, b, dc))
    return order


def attend_kernel(
    blk, n_heads, q_hbm, kv_hbm, x_hbm, w_hbm, y_hbm, q_buf, kv_buf, o_buf, x_buf, w_buf,
    w_sem, x_sem, y_sem, q_own, q_send, q_recv, kv_own, kv_send, kv_recv, o_own, o_send, o_recv,
):
    n_rounds, n_dev, tok, head_dim = q_buf.shape
    side = math.isqrt(n_dev // 2)
    me = lax.axis_index('cp')
    core = lax.rem(me, 2)
    col = lax.rem(me // 2, side)
    row = me // (2 * side)
    partner = {'cp': me + 1 - 2 * core}
    peers = [
        (lax.rem(row + dy, side) * side + lax.rem(col + dx, side)) * 2 + lax.rem(core + dc, 2)
        for dy, dx, dc in peer_offsets(side)
    ]

    def remote(src, dst, send, recv, device):
        return pltpu.make_async_remote_copy(
            src_ref=src, dst_ref=dst, send_sem=send, recv_sem=recv, device_id=device,
            device_id_type=pl.DeviceIdType.MESH,
        )

    def all_peers(r, send, recv):
        blocks = q_buf.at[r, pl.ds(0, n_dev - 1)]
        return remote(blocks, blocks, send, recv, partner)

    barrier = pltpu.get_barrier_semaphore()
    for peer in peers:
        pl.semaphore_signal(barrier, inc=1, device_id={'cp': peer}, device_id_type=pl.DeviceIdType.MESH)
    hidden = pltpu.make_async_copy(x_hbm, x_buf, x_sem)

    def keep_kv(r):
        return pltpu.make_async_copy(kv_hbm.at[:, r], kv_buf.at[r, core], kv_own.at[r])

    def share_kv(r):
        return remote(kv_hbm.at[:, r], kv_buf.at[r, core], kv_send.at[r], kv_recv.at[r], partner)

    def keep_q(r):
        return pltpu.make_async_copy(q_hbm.at[r, me], q_buf.at[r, me], q_own.at[r])

    my_rows = pl.ds(pl.multiple_of((me // n_heads) * tok, tok), tok)
    my_lanes = pl.ds(pl.multiple_of(lax.rem(me, n_heads) * head_dim, head_dim), head_dim)

    def keep_o(r):
        return pltpu.make_async_copy(q_buf.at[r, me], o_buf.at[r, my_rows, my_lanes], o_own.at[r])

    for r in range(n_rounds):
        keep_kv(r).start()
        keep_q(r).start()
    pl.semaphore_wait(barrier, n_dev - 1)
    for r in range(n_rounds):
        share_kv(r).start()
        for peer in peers:
            remote(q_hbm.at[r, peer], q_buf.at[r, me], q_send.at[r], q_recv.at[r], {'cp': peer}).start()
    hidden.start()
    n_slots, _, tile = w_buf.shape
    n_tiles = x_buf.shape[2] // tile

    def load_w(g):
        slot = lax.rem(g, n_slots)
        cols = pl.ds(pl.multiple_of(lax.rem(g, n_tiles) * tile, tile), tile)
        return pltpu.make_async_copy(w_hbm.at[:, cols], w_buf.at[slot], w_sem.at[slot])

    for g in range(n_slots):
        load_w(g).start()
    scale = (head_dim ** -0.5) * LOG2E
    group = blk // tok

    def attend(r):
        for c in range(n_dev // group):
            width = (c + 1) * blk
            mine = pl.ds(c * group, group)
            before = pl.ds(0, (c + 1) * group)
            q_blk = q_buf[r, mine].reshape(blk, head_dim)
            keys = kv_buf[r, 0, before].reshape(width, head_dim)
            vals = kv_buf[r, 1, before].reshape(width, head_dim)
            scores = lax.dot_general(q_blk, keys, (((1,), (1,)), ((), ())), preferred_element_type=jnp.float32)
            row_ids = lax.broadcasted_iota(jnp.int32, (blk, width), 0) + c * blk
            col_ids = lax.broadcasted_iota(jnp.int32, (blk, width), 1)
            scores = jnp.where(col_ids <= row_ids, scores, -jnp.inf)
            row_max = jnp.max(scores, axis=1, keepdims=True)
            p_weights = jnp.exp2((scores - row_max) * scale)
            row_sum = jnp.sum(p_weights, axis=1, keepdims=True)
            out = jnp.dot(p_weights.astype(jnp.bfloat16), vals, preferred_element_type=jnp.float32)
            q_buf[r, mine] = (out / row_sum).astype(q_buf.dtype).reshape(group, tok, head_dim)

    def project_out(r):
        all_peers(r, o_send.at[r], o_recv.at[r]).wait_recv()
        keep_o(r).wait()

        @pl.loop(0, n_tiles)
        def _(t):
            g = r * n_tiles + t
            cols = pl.ds(pl.multiple_of(t * tile, tile), tile)
            load_w(g).wait()
            proj = jnp.dot(o_buf[r], w_buf[lax.rem(g, n_slots)], preferred_element_type=jnp.float32)
            x_buf[r, :, cols] = (x_buf[r, :, cols].astype(jnp.float32) + proj).astype(x_buf.dtype)

            @pl.when(g + n_slots < n_rounds * n_tiles)
            def _():
                load_w(g + n_slots).start()

        pltpu.make_async_copy(x_buf.at[r], y_hbm.at[r], y_sem.at[r]).start()

    @pl.loop(0, n_rounds)
    def _(r):
        keep_kv(r).wait()
        share_kv(r).wait_recv()
        keep_q(r).wait()
        all_peers(r, q_send.at[r], q_recv.at[r]).wait_recv()
        attend(r)
        keep_o(r).start()
        for peer in peers:
            remote(q_buf.at[r, peer], o_buf.at[r, my_rows, my_lanes], o_send.at[r], o_recv.at[r], {'cp': peer}).start()

        @pl.when(r == 0)
        def _():
            hidden.wait()

        @pl.when(r > 0)
        def _():
            project_out(r - 1)

    project_out(n_rounds - 1)
    for r in range(n_rounds):
        share_kv(r).wait_send()
        all_peers(r, q_send.at[r], q_recv.at[r]).wait_send()
        all_peers(r, o_send.at[r], o_recv.at[r]).wait_send()
        pltpu.make_async_copy(x_buf.at[r], y_hbm.at[r], y_sem.at[r]).wait()


def attend(queries, kv_mine, hidden, w_o, n_heads):
    n_rounds, n_dev, tok, head_dim = queries.shape
    rows, width = hidden.shape[1:]
    blk = 4 * tok
    dma = pltpu.SemaphoreType.DMA
    return pl.pallas_call(
        functools.partial(attend_kernel, blk, n_heads),
        out_shape=jax.ShapeDtypeStruct(hidden.shape, hidden.dtype),
        in_specs=[pl.BlockSpec(memory_space=pl.ANY)] * 4,
        out_specs=pl.BlockSpec(memory_space=pl.ANY),
        scratch_shapes=[
            pltpu.VMEM((n_rounds, n_dev, tok, head_dim), jnp.bfloat16),
            pltpu.VMEM((n_rounds, 2, n_dev, tok, head_dim), jnp.bfloat16),
            pltpu.VMEM((n_rounds, rows, n_heads * head_dim), jnp.bfloat16),
            pltpu.VMEM((n_rounds, rows, width), jnp.bfloat16),
            pltpu.VMEM((4, w_o.shape[0], 512), jnp.bfloat16),
            dma((4,)),
            dma,
        ] + [dma((n_rounds,))] * 10,
        compiler_params=pltpu.CompilerParams(collective_id=0, has_side_effects=True, vmem_limit_bytes=66 * 1000 * 1000),
        cost_estimate=pl.CostEstimate(flops=10 ** 11, bytes_accessed=10 ** 8, transcendentals=10 ** 7),
        name='attend',
    )(queries, kv_mine, hidden, w_o)


def solution(mesh):
    cp_size = mesh.shape['cp']

    def per_device(hidden, positions, w_q, w_k, w_v, w_o):
        n_seq, tok_dev, width = hidden.shape
        n_heads, head_dim = w_q.shape[1], w_q.shape[2]
        n_kv = w_k.shape[1]
        per_round = cp_size // n_heads
        n_rounds = n_seq // per_round
        cos_tab, sin_tab = rope_tables(positions, head_dim)
        k_rot = rope_apply(project(hidden, w_k), cos_tab, sin_tab)
        values = project(hidden, w_v)
        kv_all = jnp.stack([k_rot, values]).reshape(2, n_rounds, per_round, tok_dev, n_kv, head_dim)
        kv_send = kv_all.transpose(2, 4, 0, 1, 3, 5).reshape(cp_size, n_rounds, tok_dev, head_dim)
        kv_mine = lax.all_to_all(kv_send, 'cp', 0, 0)
        late, _ = lax.optimization_barrier((hidden, kv_send))
        queries = rope_apply(project(late, w_q), cos_tab, sin_tab)
        queries = queries.transpose(0, 2, 1, 3).reshape(n_rounds, cp_size, tok_dev, head_dim)
        rows = per_round * tok_dev
        out = attend(queries, kv_mine, hidden.reshape(n_rounds, rows, width), w_o.reshape(n_heads * head_dim, width), n_heads)
        return out.reshape(n_seq, tok_dev, width)

    rep_spec = P(None, None, None)
    return jax.shard_map(per_device, mesh=mesh, in_specs=(P('dp', 'cp', None), P('dp', 'cp'), rep_spec, rep_spec, rep_spec, rep_spec), out_specs=P('dp', 'cp', None), check_vma=False)
```

```python
import functools
import math

import jax
import jax.numpy as jnp
from jax import lax
from jax.experimental import pallas as pl
from jax.experimental.pallas import tpu as pltpu
from jax.sharding import PartitionSpec as P

ROPE_BASE = 500000.0
LOG2E = 1.4426950408889634


def rope_tables(positions, head_dim):
    inv_freq = ROPE_BASE ** (-jnp.arange(0, head_dim, 2, dtype=jnp.float32) / head_dim)
    angles = positions.astype(jnp.float32)[..., None] * inv_freq
    angles = jnp.concatenate([angles, angles], axis=-1)
    return jnp.cos(angles)[:, :, None, :], jnp.sin(angles)[:, :, None, :]


def rope_apply(in_vals, cos_tab, sin_tab):
    half_dim = in_vals.shape[-1] // 2
    val_f32 = in_vals.astype(jnp.float32)
    rotated = jnp.concatenate([-val_f32[..., half_dim:], val_f32[..., :half_dim]], axis=-1)
    return (val_f32 * cos_tab + rotated * sin_tab).astype(jnp.bfloat16)


def project(hidden, weights):
    return jnp.einsum('bsd,dhe->bshe', hidden, weights, preferred_element_type=jnp.float32).astype(jnp.bfloat16)


def peer_offsets(side):
    order = []
    for dy in range(side):
        for dx in range(side):
            for dc in range(2):
                for a, b in ((dy, dx), (-dy % side, -dx % side), (dx, dy), (-dx % side, -dy % side)):
                    if (a, b, dc) != (0, 0, 0) and (a, b, dc) not in order:
                        order.append((a, b, dc))
    return sorted(order, key=lambda t: -(min(t[0], side - t[0]) + min(t[1], side - t[1])))


def attend_kernel(
    blk, n_heads, q_hbm, k_hbm, v_hbm, x_hbm, w_hbm, y_hbm, q_buf, kv_buf, o_buf, x_buf, w_buf,
    w_sem, x_sem, y_sem, q_own, q_send, q_recv, kv_own, kv_send, kv_recv, o_own, o_send, o_recv,
):
    n_rounds, n_dev, tok, head_dim = q_buf.shape
    side = math.isqrt(n_dev // 2)
    me = lax.axis_index('cp')
    core = lax.rem(me, 2)
    col = lax.rem(me // 2, side)
    row = me // (2 * side)
    partner = {'cp': me + 1 - 2 * core}
    peers = [
        (lax.rem(row + dy, side) * side + lax.rem(col + dx, side)) * 2 + lax.rem(core + dc, 2)
        for dy, dx, dc in peer_offsets(side)
    ]

    def remote(src, dst, send, recv, device):
        return pltpu.make_async_remote_copy(
            src_ref=src, dst_ref=dst, send_sem=send, recv_sem=recv, device_id=device,
            device_id_type=pl.DeviceIdType.MESH,
        )

    def all_peers(r, send, recv):
        blocks = q_buf.at[r, pl.ds(0, n_dev - 1)]
        return remote(blocks, blocks, send, recv, partner)

    barrier = pltpu.get_barrier_semaphore()
    for peer in peers:
        pl.semaphore_signal(barrier, inc=1, device_id={'cp': peer}, device_id_type=pl.DeviceIdType.MESH)
    hidden = pltpu.make_async_copy(x_hbm, x_buf, x_sem)

    half = pl.ds(pl.multiple_of(core * (tok // 2), tok // 2), tok // 2)
    kv_hbm = (k_hbm, v_hbm)

    def keep_kv(r, a):
        return pltpu.make_async_copy(kv_hbm[a].at[:, r], kv_buf.at[r, a, :, half], kv_own.at[2 * r + a])

    def share_kv(r, a):
        sems = kv_send.at[2 * r + a], kv_recv.at[2 * r + a]
        return remote(kv_hbm[a].at[:, r], kv_buf.at[r, a, :, half], *sems, partner)

    def keep_q(r):
        return pltpu.make_async_copy(q_hbm.at[r, me], q_buf.at[r, me], q_own.at[r])

    my_rows = pl.ds(pl.multiple_of((me // n_heads) * tok, tok), tok)
    my_lanes = pl.ds(pl.multiple_of(lax.rem(me, n_heads) * head_dim, head_dim), head_dim)

    def keep_o(r):
        return pltpu.make_async_copy(q_buf.at[r, me], o_buf.at[r, my_rows, my_lanes], o_own.at[r])

    for r in range(n_rounds):
        for a in range(2):
            keep_kv(r, a).start()
        keep_q(r).start()
    pl.semaphore_wait(barrier, n_dev - 1)
    for r in range(n_rounds):
        for a in range(2):
            share_kv(r, a).start()
        for peer in peers:
            remote(q_hbm.at[r, peer], q_buf.at[r, me], q_send.at[r], q_recv.at[r], {'cp': peer}).start()
    hidden.start()
    n_slots, _, tile = w_buf.shape
    n_tiles = x_buf.shape[2] // tile

    def load_w(g):
        slot = lax.rem(g, n_slots)
        cols = pl.ds(pl.multiple_of(lax.rem(g, n_tiles) * tile, tile), tile)
        return pltpu.make_async_copy(w_hbm.at[:, cols], w_buf.at[slot], w_sem.at[slot])

    for g in range(n_slots):
        load_w(g).start()
    scale = (head_dim ** -0.5) * LOG2E
    group = blk // tok

    def attend(r):
        for c in range(n_dev // group):
            width = (c + 1) * blk
            mine = pl.ds(c * group, group)
            before = pl.ds(0, (c + 1) * group)
            q_blk = q_buf[r, mine].reshape(blk, head_dim)
            keys = kv_buf[r, 0, before].reshape(width, head_dim)
            vals = kv_buf[r, 1, before].reshape(width, head_dim)
            scores = lax.dot_general(q_blk, keys, (((1,), (1,)), ((), ())), preferred_element_type=jnp.float32)
            row_ids = lax.broadcasted_iota(jnp.int32, (blk, width), 0) + c * blk
            col_ids = lax.broadcasted_iota(jnp.int32, (blk, width), 1)
            scores = jnp.where(col_ids <= row_ids, scores, -jnp.inf)
            row_max = jnp.max(scores, axis=1, keepdims=True)
            p_weights = jnp.exp2((scores - row_max) * scale)
            row_sum = jnp.sum(p_weights, axis=1, keepdims=True)
            out = jnp.dot(p_weights.astype(jnp.bfloat16), vals, preferred_element_type=jnp.float32)
            q_buf[r, mine] = (out / row_sum).astype(q_buf.dtype).reshape(group, tok, head_dim)

    def project_out(r):
        all_peers(r, o_send.at[r], o_recv.at[r]).wait_recv()
        keep_o(r).wait()

        @pl.loop(0, n_tiles)
        def _(t):
            g = r * n_tiles + t
            cols = pl.ds(pl.multiple_of(t * tile, tile), tile)
            load_w(g).wait()
            proj = jnp.dot(o_buf[r], w_buf[lax.rem(g, n_slots)], preferred_element_type=jnp.float32)
            x_buf[r, :, cols] = (x_buf[r, :, cols].astype(jnp.float32) + proj).astype(x_buf.dtype)

            @pl.when(g + n_slots < n_rounds * n_tiles)
            def _():
                load_w(g + n_slots).start()

        pltpu.make_async_copy(x_buf.at[r], y_hbm.at[r], y_sem.at[r]).start()

    @pl.loop(0, n_rounds)
    def _(r):
        for a in range(2):
            keep_kv(r, a).wait()
            share_kv(r, a).wait_recv()
        keep_q(r).wait()
        all_peers(r, q_send.at[r], q_recv.at[r]).wait_recv()
        attend(r)
        keep_o(r).start()
        for peer in peers:
            remote(q_buf.at[r, peer], o_buf.at[r, my_rows, my_lanes], o_send.at[r], o_recv.at[r], {'cp': peer}).start()

        @pl.when(r == 0)
        def _():
            hidden.wait()

        @pl.when(r > 0)
        def _():
            project_out(r - 1)

    project_out(n_rounds - 1)
    for r in range(n_rounds):
        for a in range(2):
            share_kv(r, a).wait_send()
        all_peers(r, q_send.at[r], q_recv.at[r]).wait_send()
        all_peers(r, o_send.at[r], o_recv.at[r]).wait_send()
        pltpu.make_async_copy(x_buf.at[r], y_hbm.at[r], y_sem.at[r]).wait()


def attend(queries, k_mine, v_mine, hidden, w_o, n_heads):
    n_rounds, n_dev, tok, head_dim = queries.shape
    rows, width = hidden.shape[1:]
    blk = 4 * tok
    dma = pltpu.SemaphoreType.DMA
    return pl.pallas_call(
        functools.partial(attend_kernel, blk, n_heads),
        out_shape=jax.ShapeDtypeStruct(hidden.shape, hidden.dtype),
        in_specs=[pl.BlockSpec(memory_space=pl.ANY)] * 5,
        out_specs=pl.BlockSpec(memory_space=pl.ANY),
        scratch_shapes=[
            pltpu.VMEM((n_rounds, n_dev, tok, head_dim), jnp.bfloat16),
            pltpu.VMEM((n_rounds, 2, n_dev, tok, head_dim), jnp.bfloat16),
            pltpu.VMEM((n_rounds, rows, n_heads * head_dim), jnp.bfloat16),
            pltpu.VMEM((n_rounds, rows, width), jnp.bfloat16),
            pltpu.VMEM((4, w_o.shape[0], 512), jnp.bfloat16),
            dma((4,)),
            dma,
        ] + [dma((n_rounds,))] * 4 + [dma((2 * n_rounds,))] * 3 + [dma((n_rounds,))] * 3,
        compiler_params=pltpu.CompilerParams(collective_id=0, has_side_effects=True, vmem_limit_bytes=66 * 1000 * 1000),
        cost_estimate=pl.CostEstimate(flops=10 ** 11, bytes_accessed=10 ** 8, transcendentals=10 ** 7),
        name='attend',
    )(queries, k_mine, v_mine, hidden, w_o)


def solution(mesh):
    cp_size = mesh.shape['cp']

    def per_device(hidden, positions, w_q, w_k, w_v, w_o):
        n_seq, tok_dev, width = hidden.shape
        n_heads, head_dim = w_q.shape[1], w_q.shape[2]
        n_kv = w_k.shape[1]
        per_round = cp_size // n_heads
        n_rounds = n_seq // per_round
        cos_tab, sin_tab = rope_tables(positions, head_dim)

        def exchange_halves(heads):
            parts = heads.reshape(n_rounds, per_round, 2, tok_dev // 2, n_kv, head_dim)
            send = parts.transpose(1, 4, 2, 0, 3, 5).reshape(cp_size, n_rounds, tok_dev // 2, head_dim)
            return send, lax.all_to_all(send, 'cp', 0, 0)

        v_send, v_mine = exchange_halves(project(hidden, w_v))
        late, _ = lax.optimization_barrier((hidden, v_send))
        k_send, k_mine = exchange_halves(rope_apply(project(late, w_k), cos_tab, sin_tab))
        late, _ = lax.optimization_barrier((hidden, k_send))
        queries = rope_apply(project(late, w_q), cos_tab, sin_tab)
        queries = queries.transpose(0, 2, 1, 3).reshape(n_rounds, cp_size, tok_dev, head_dim)
        rows = per_round * tok_dev
        out = attend(queries, k_mine, v_mine, hidden.reshape(n_rounds, rows, width), w_o.reshape(n_heads * head_dim, width), n_heads)
        return out.reshape(n_seq, tok_dev, width)

    rep_spec = P(None, None, None)
    return jax.shard_map(per_device, mesh=mesh, in_specs=(P('dp', 'cp', None), P('dp', 'cp'), rep_spec, rep_spec, rep_spec, rep_spec), out_specs=P('dp', 'cp', None), check_vma=False)
```

```python
import functools
import math

import jax
import jax.numpy as jnp
from jax import lax
from jax.experimental import pallas as pl
from jax.experimental.pallas import tpu as pltpu
from jax.sharding import PartitionSpec as P

ROPE_BASE = 500000.0
LOG2E = 1.4426950408889634


def rope_tables(positions, head_dim):
    inv_freq = ROPE_BASE ** (-jnp.arange(0, head_dim, 2, dtype=jnp.float32) / head_dim)
    angles = positions.astype(jnp.float32)[..., None] * inv_freq
    angles = jnp.concatenate([angles, angles], axis=-1)
    return jnp.cos(angles)[:, :, None, :], jnp.sin(angles)[:, :, None, :]


def rope_apply(in_vals, cos_tab, sin_tab):
    half_dim = in_vals.shape[-1] // 2
    val_f32 = in_vals.astype(jnp.float32)
    rotated = jnp.concatenate([-val_f32[..., half_dim:], val_f32[..., :half_dim]], axis=-1)
    return (val_f32 * cos_tab + rotated * sin_tab).astype(jnp.bfloat16)


def project(hidden, weights):
    return jnp.einsum('bsd,dhe->bshe', hidden, weights, preferred_element_type=jnp.float32).astype(jnp.bfloat16)


def peer_offsets(side):
    order = []
    for dy in range(side):
        for dx in range(side):
            for dc in range(2):
                for a, b in ((dy, dx), (-dy % side, -dx % side), (dx, dy), (-dx % side, -dy % side)):
                    if (a, b, dc) != (0, 0, 0) and (a, b, dc) not in order:
                        order.append((a, b, dc))
    return sorted(order, key=lambda t: -(min(t[0], side - t[0]) + min(t[1], side - t[1])))


def attend_kernel(
    blk, n_heads, q_hbm, k_hbm, v_hbm, x_hbm, w_hbm, y_hbm, q_buf, kv_buf, o_buf, x_buf, w_buf,
    w_sem, x_sem, y_sem, q_own, q_send, q_recv, kv_own, kv_send, kv_recv, o_own, o_send, o_recv,
):
    n_rounds, n_dev, tok, head_dim = q_buf.shape
    side = math.isqrt(n_dev // 2)
    me = lax.axis_index('cp')
    core = lax.rem(me, 2)
    col = lax.rem(me // 2, side)
    row = me // (2 * side)
    partner = {'cp': me + 1 - 2 * core}
    peers = [
        (lax.rem(row + dy, side) * side + lax.rem(col + dx, side)) * 2 + lax.rem(core + dc, 2)
        for dy, dx, dc in peer_offsets(side)
    ]

    def remote(src, dst, send, recv, device):
        return pltpu.make_async_remote_copy(
            src_ref=src, dst_ref=dst, send_sem=send, recv_sem=recv, device_id=device,
            device_id_type=pl.DeviceIdType.MESH,
        )

    def all_peers(r, send, recv):
        blocks = q_buf.at[r, pl.ds(0, n_dev - 1)]
        return remote(blocks, blocks, send, recv, partner)

    barrier = pltpu.get_barrier_semaphore()
    for peer in peers:
        pl.semaphore_signal(barrier, inc=1, device_id={'cp': peer}, device_id_type=pl.DeviceIdType.MESH)
    hidden = pltpu.make_async_copy(x_hbm, x_buf, x_sem)

    half = pl.ds(pl.multiple_of(core * (tok // 2), tok // 2), tok // 2)
    kv_hbm = (k_hbm, v_hbm)

    def keep_kv(r, a):
        return pltpu.make_async_copy(kv_hbm[a].at[:, r], kv_buf.at[r, a, :, half], kv_own.at[2 * r + a])

    def share_kv(r, a):
        sems = kv_send.at[2 * r + a], kv_recv.at[2 * r + a]
        return remote(kv_hbm[a].at[:, r], kv_buf.at[r, a, :, half], *sems, partner)

    def keep_q(r):
        return pltpu.make_async_copy(q_hbm.at[r, me], q_buf.at[r, me], q_own.at[r])

    my_rows = pl.ds(pl.multiple_of((me // n_heads) * tok, tok), tok)
    my_lanes = pl.ds(pl.multiple_of(lax.rem(me, n_heads) * head_dim, head_dim), head_dim)

    def keep_o(r):
        return pltpu.make_async_copy(q_buf.at[r, me], o_buf.at[r, my_rows, my_lanes], o_own.at[r])

    for r in range(n_rounds):
        for a in range(2):
            keep_kv(r, a).start()
        keep_q(r).start()
    pl.semaphore_wait(barrier, n_dev - 1)
    for r in range(n_rounds):
        for a in range(2):
            share_kv(r, a).start()
        for peer in peers:
            remote(q_hbm.at[r, peer], q_buf.at[r, me], q_send.at[r], q_recv.at[r], {'cp': peer}).start()
    hidden.start()
    n_slots, _, tile = w_buf.shape
    n_tiles = x_buf.shape[2] // tile

    def load_w(g):
        slot = lax.rem(g, n_slots)
        cols = pl.ds(pl.multiple_of(lax.rem(g, n_tiles) * tile, tile), tile)
        return pltpu.make_async_copy(w_hbm.at[:, cols], w_buf.at[slot], w_sem.at[slot])

    for g in range(n_slots):
        load_w(g).start()
    scale = (head_dim ** -0.5) * LOG2E
    group = blk // tok

    def attend(r):
        for c in range(n_dev // group):
            width = (c + 1) * blk
            mine = pl.ds(c * group, group)
            before = pl.ds(0, (c + 1) * group)
            q_blk = q_buf[r, mine].reshape(blk, head_dim)
            keys = kv_buf[r, 0, before].reshape(width, head_dim)
            vals = kv_buf[r, 1, before].reshape(width, head_dim)
            scores = lax.dot_general(q_blk, keys, (((1,), (1,)), ((), ())), preferred_element_type=jnp.float32)
            row_ids = lax.broadcasted_iota(jnp.int32, (blk, width), 0) + c * blk
            col_ids = lax.broadcasted_iota(jnp.int32, (blk, width), 1)
            scores = jnp.where(col_ids <= row_ids, scores, -jnp.inf)
            row_max = jnp.max(scores, axis=1, keepdims=True)
            p_weights = jnp.exp2((scores - row_max) * scale)
            row_sum = jnp.sum(p_weights, axis=1, keepdims=True)
            out = jnp.dot(p_weights.astype(jnp.bfloat16), vals, preferred_element_type=jnp.float32)
            q_buf[r, mine] = (out / row_sum).astype(q_buf.dtype).reshape(group, tok, head_dim)

    def project_out(r):
        all_peers(r, o_send.at[r], o_recv.at[r]).wait_recv()
        keep_o(r).wait()

        @pl.loop(0, n_tiles)
        def _(t):
            g = r * n_tiles + t
            cols = pl.ds(pl.multiple_of(t * tile, tile), tile)
            load_w(g).wait()
            proj = jnp.dot(o_buf[r], w_buf[lax.rem(g, n_slots)], preferred_element_type=jnp.float32)
            x_buf[r, :, cols] = (x_buf[r, :, cols].astype(jnp.float32) + proj).astype(x_buf.dtype)

            @pl.when(g + n_slots < n_rounds * n_tiles)
            def _():
                load_w(g + n_slots).start()

        pltpu.make_async_copy(x_buf.at[r], y_hbm.at[r], y_sem.at[r]).start()

    def send_o(r):
        keep_o(r).start()
        for peer in peers:
            remote(q_buf.at[r, peer], o_buf.at[r, my_rows, my_lanes], o_send.at[r], o_recv.at[r], {'cp': peer}).start()

    @pl.loop(0, n_rounds)
    def _(r):
        for a in range(2):
            keep_kv(r, a).wait()
            share_kv(r, a).wait_recv()
        keep_q(r).wait()
        all_peers(r, q_send.at[r], q_recv.at[r]).wait_recv()
        attend(r)

        @pl.when(r == n_rounds - 2)
        def _():
            for q in range(n_rounds):
                all_peers(q, q_send.at[q], q_recv.at[q]).wait_send()
            for q in range(n_rounds - 1):
                send_o(q)

        @pl.when(r == n_rounds - 1)
        def _():
            send_o(r)

    hidden.wait()
    pl.loop(0, n_rounds)(project_out)
    for r in range(n_rounds):
        for a in range(2):
            share_kv(r, a).wait_send()
        all_peers(r, o_send.at[r], o_recv.at[r]).wait_send()
        pltpu.make_async_copy(x_buf.at[r], y_hbm.at[r], y_sem.at[r]).wait()


def attend(queries, k_mine, v_mine, hidden, w_o, n_heads):
    n_rounds, n_dev, tok, head_dim = queries.shape
    rows, width = hidden.shape[1:]
    blk = 4 * tok
    dma = pltpu.SemaphoreType.DMA
    return pl.pallas_call(
        functools.partial(attend_kernel, blk, n_heads),
        out_shape=jax.ShapeDtypeStruct(hidden.shape, hidden.dtype),
        in_specs=[pl.BlockSpec(memory_space=pl.ANY)] * 5,
        out_specs=pl.BlockSpec(memory_space=pl.ANY),
        scratch_shapes=[
            pltpu.VMEM((n_rounds, n_dev, tok, head_dim), jnp.bfloat16),
            pltpu.VMEM((n_rounds, 2, n_dev, tok, head_dim), jnp.bfloat16),
            pltpu.VMEM((n_rounds, rows, n_heads * head_dim), jnp.bfloat16),
            pltpu.VMEM((n_rounds, rows, width), jnp.bfloat16),
            pltpu.VMEM((4, w_o.shape[0], 512), jnp.bfloat16),
            dma((4,)),
            dma,
        ] + [dma((n_rounds,))] * 4 + [dma((2 * n_rounds,))] * 3 + [dma((n_rounds,))] * 3,
        compiler_params=pltpu.CompilerParams(collective_id=0, has_side_effects=True, vmem_limit_bytes=66 * 1000 * 1000),
        cost_estimate=pl.CostEstimate(flops=10 ** 11, bytes_accessed=10 ** 8, transcendentals=10 ** 7),
        name='attend',
    )(queries, k_mine, v_mine, hidden, w_o)


def solution(mesh):
    cp_size = mesh.shape['cp']

    def per_device(hidden, positions, w_q, w_k, w_v, w_o):
        n_seq, tok_dev, width = hidden.shape
        n_heads, head_dim = w_q.shape[1], w_q.shape[2]
        n_kv = w_k.shape[1]
        per_round = cp_size // n_heads
        n_rounds = n_seq // per_round
        cos_tab, sin_tab = rope_tables(positions, head_dim)

        def exchange_halves(heads):
            parts = heads.reshape(n_rounds, per_round, 2, tok_dev // 2, n_kv, head_dim)
            send = parts.transpose(1, 4, 2, 0, 3, 5).reshape(cp_size, n_rounds, tok_dev // 2, head_dim)
            return send, lax.all_to_all(send, 'cp', 0, 0)

        v_send, v_mine = exchange_halves(project(hidden, w_v))
        late, _ = lax.optimization_barrier((hidden, v_send))
        k_send, k_mine = exchange_halves(rope_apply(project(late, w_k), cos_tab, sin_tab))
        late, _ = lax.optimization_barrier((hidden, k_send))
        queries = rope_apply(project(late, w_q), cos_tab, sin_tab)
        queries = queries.transpose(0, 2, 1, 3).reshape(n_rounds, cp_size, tok_dev, head_dim)
        rows = per_round * tok_dev
        out = attend(queries, k_mine, v_mine, hidden.reshape(n_rounds, rows, width), w_o.reshape(n_heads * head_dim, width), n_heads)
        return out.reshape(n_seq, tok_dev, width)

    rep_spec = P(None, None, None)
    return jax.shard_map(per_device, mesh=mesh, in_specs=(P('dp', 'cp', None), P('dp', 'cp'), rep_spec, rep_spec, rep_spec, rep_spec), out_specs=P('dp', 'cp', None), check_vma=False)
```
